32 devices in a mesh: gx: 4 (over z), gy: 4 (over y, x), gz: 2 (over core).
Axes of the slice: x: 2, y: 2, z: 4, core: 2. Of those that a mesh axis runs over, the one named last changes fastest.
Arguments:
- eigvecs: bfloat16 [64, 32, 96, 512], P('gx', 'gy', 'gz'), may hold values from -7 to 7, as said below
- material: float32 [2, 64, 32, 96], P(None, 'gx', 'gy', 'gz'), may hold values from 0.5 to 2
Outputs:
- stiffness: float32 [512, 512], P(('gx', 'gy', 'gz'))
- mass_matrix: float32 [512, 512], P(('gx', 'gy', 'gz'))
The draws below stay inside these ranges and needn't reach their ends.
Inputs may be any that keep to these rules, and one draw needn't show every extreme that they name: `eigvecs`: entries are a rough part plus a part that varies slowly over the grid.
All inputs are finite; a program needn't handle non-finite values.
Results may differ from the reference program's by a relative error of at most 0.0003.
Values may be sent and summed in bfloat16 or wider, within the bound.
A program may use at most 128 MiB of HBM per device.

```python
import math
import jax
import jax.numpy as jnp
from jax import lax

K = 512
NX = 64
NY = 32
NZ = 96


def draw_eigvecs(key, part):
    keys = jax.random.split(key, 7)
    rough = jnp.clip(jax.random.normal(keys[0], (NX, NY, NZ, K), jnp.float32), -4.0, 4.0)
    amplitude = 2.0
    freq_x = jax.random.randint(keys[1], (K,), 1, 4).astype(jnp.float32)
    freq_y = jax.random.randint(keys[2], (K,), 1, 4).astype(jnp.float32)
    freq_z = jax.random.randint(keys[3], (K,), 1, 4).astype(jnp.float32)
    phase_x = jax.random.uniform(keys[4], (K,), jnp.float32)
    phase_y = jax.random.uniform(keys[5], (K,), jnp.float32)
    phase_z = jax.random.uniform(keys[6], (K,), jnp.float32)
    coord_x = jnp.arange(NX, dtype=jnp.float32)[:, None] / NX
    coord_y = jnp.arange(NY, dtype=jnp.float32)[:, None] / NY
    coord_z = jnp.arange(NZ, dtype=jnp.float32)[:, None] / NZ
    wave_x = jnp.cos(2.0 * jnp.pi * (coord_x * freq_x + phase_x))
    wave_y = jnp.cos(2.0 * jnp.pi * (coord_y * freq_y + phase_y))
    wave_z = jnp.cos(2.0 * jnp.pi * (coord_z * freq_z + phase_z))
    smooth = wave_x[:, None, None, :] * wave_y[None, :, None, :] * wave_z[None, None, :, :]
    return (rough + amplitude * smooth).astype(jnp.bfloat16)


def shard_levels(own_key, shape, cuts, low, top_value):
    factor_of = 1.0
    for dim, shards_of in cuts:
        heights = jax.random.uniform(jax.random.fold_in(jax.random.fold_in(own_key, 6), dim), (shards_of,), jnp.float32, low / len(cuts), top_value / len(cuts))
        factor_of = factor_of * jnp.repeat(jnp.exp(heights), shape[dim] // shards_of).reshape((-1,) + (1,) * (len(shape) - 1 - dim))
    return factor_of


def setup_inputs(seed: int = 0) -> dict:
    streams_of = jax.random.split(jax.random.key(seed), 3)
    eigvecs = draw_eigvecs(jax.random.fold_in(streams_of[2], 71), 0)
    material = jnp.clip(jnp.exp(math.log(2.0) - 1.3862944 * jax.random.uniform(streams_of[1], (2, NX, NY, NZ), jnp.float32) ** shard_levels(streams_of[1], (2, NX, NY, NZ), ((1, 4), (2, 4), (3, 2)), -0.2, 0.2)), 0.5, 2.0)
    return {"eigvecs": eigvecs, "material": material}


stencil_offsets = [(dx, dy, dz) for dx in (-1, 0, 1) for dy in (-1, 0, 1) for dz in (-1, 0, 1) if (dx, dy, dz) != (0, 0, 0)]


def coupling(offset):
    nonzero = sum(abs(entry) for entry in offset)
    return 0.25 * 0.5 ** (nonzero - 1)


def mass_weight(offset):
    weight = 1.0
    for entry in offset:
        weight = weight * (4.0 / 6.0 if entry == 0 else 1.0 / 6.0)
    return weight


def apply_operators(padded, padded_material):
    size_x = padded.shape[0] - 2
    size_y = padded.shape[1] - 2
    size_z = padded.shape[2] - 2
    centre = padded[1:-1, 1:-1, 1:-1].astype(jnp.float32)
    kappa_centre = padded_material[0, 1:-1, 1:-1, 1:-1]
    rho_centre = padded_material[1, 1:-1, 1:-1, 1:-1]
    stiff_sum = jnp.zeros(centre.shape, jnp.float32)
    mass_sum = mass_weight((0, 0, 0)) * rho_centre[..., None] * centre
    for offset in stencil_offsets:
        lower = (1 + offset[0], 1 + offset[1], 1 + offset[2])
        shifted = padded[lower[0]:lower[0] + size_x, lower[1]:lower[1] + size_y, lower[2]:lower[2] + size_z].astype(jnp.float32)
        kappa_side = padded_material[0, lower[0]:lower[0] + size_x, lower[1]:lower[1] + size_y, lower[2]:lower[2] + size_z]
        rho_side = padded_material[1, lower[0]:lower[0] + size_x, lower[1]:lower[1] + size_y, lower[2]:lower[2] + size_z]
        stiff_sum = stiff_sum + (coupling(offset) * 0.5 * (kappa_centre + kappa_side))[..., None] * (centre - shifted)
        mass_sum = mass_sum + (mass_weight(offset) * 0.5 * (rho_centre + rho_side))[..., None] * shifted
    return stiff_sum.astype(jnp.bfloat16), mass_sum.astype(jnp.bfloat16)


def reference(eigvecs, material):
    cells = NX * NY * NZ
    block_cols = 32
    padded_material = jnp.pad(material, ((0, 0), (1, 1), (1, 1), (1, 1)))
    flat_vectors = eigvecs.reshape(cells, K)

    def column_block(block_index):
        first_col = block_index * block_cols
        col_block = lax.dynamic_slice_in_dim(eigvecs, first_col, block_cols, 3)
        padded = jnp.pad(col_block, ((1, 1), (1, 1), (1, 1), (0, 0)))
        stiff_vecs, mass_vecs = apply_operators(padded, padded_material)
        dims = (((0,), (0,)), ((), ()))
        stiff_cols = lax.dot_general(flat_vectors, stiff_vecs.reshape(cells, block_cols), dims, preferred_element_type=jnp.float32)
        mass_cols = lax.dot_general(flat_vectors, mass_vecs.reshape(cells, block_cols), dims, preferred_element_type=jnp.float32)
        return stiff_cols, mass_cols

    stiff_blocks, mass_blocks = lax.map(column_block, jnp.arange(K // block_cols, dtype=jnp.int32))
    stiffness = jnp.transpose(stiff_blocks, (1, 0, 2)).reshape(K, K) / cells
    mass_matrix = jnp.transpose(mass_blocks, (1, 0, 2)).reshape(K, K) / cells
    return stiffness, mass_matrix
```

```python
import functools
import numpy as np
import jax
import jax.numpy as jnp
from jax import lax
from jax.experimental import pallas as pl
from jax.experimental.pallas import tpu as pltpu
from jax.sharding import PartitionSpec as P


def upper(cells, axis, dim):
    count = lax.axis_size(axis)
    head = lax.slice_in_dim(cells, 0, 1, axis=dim)
    return lax.ppermute(head, axis, [(i + 1, i) for i in range(count - 1)])


def taps(count, middle):
    t = middle * np.eye(count) + np.eye(count, k=1) + np.eye(count, k=-1)
    t[-1, -1] = 0.0
    return t


def rows_of(size_y, size_z):
    order = np.zeros((size_y + 1, size_z + 1), np.int64)
    for y in range(size_y + 1):
        order[y, :size_z] = y * size_z + np.arange(size_z)
        order[y, size_z] = (size_y + 1) * size_z + y
    return order


def plane_matrix(size_y, size_z, rows):
    order = rows_of(size_y, size_z).reshape(-1)
    blocks = []
    for middle in (2.0, 4.0):
        full = np.kron(taps(size_y + 1, middle), taps(size_z + 1, middle))
        block = np.zeros((rows, rows))
        block[np.ix_(order, order)] = full
        blocks.append(block)
    return np.concatenate(blocks, 0)


def coefficients(ext, rows, cells_shape):
    size_x, size_y, size_z = cells_shape
    kappa, rho = ext[0], ext[1]
    field = kappa
    for dim in range(3):
        n = field.shape[dim]
        pad = [(1, 1) if d == dim else (0, 0) for d in range(3)]
        wide = jnp.pad(field, pad)
        lower = lax.slice_in_dim(wide, 0, n, axis=dim)
        above = lax.slice_in_dim(wide, 2, n + 2, axis=dim)
        shape = [1, 1, 1]
        shape[dim] = n
        diag = jnp.asarray(np.r_[np.full(n - 1, 2.0), 0.0].reshape(shape), jnp.float32)
        field = lower + above + diag * field
    owned = np.zeros(kappa.shape, np.float32)
    owned[:size_x, :size_y, :size_z] = 2.0
    diag = owned * kappa + field * (1.0 / 32.0)
    parts = jnp.stack([diag, kappa * (1.0 / 16.0), rho * (1.0 / 216.0)], axis=1)
    main = parts[..., :size_z].reshape(size_x + 1, 3, (size_y + 1) * size_z)
    edge = parts[..., size_z]
    both = jnp.concatenate([main, edge], axis=2)
    return jnp.pad(both, ((0, 0), (0, 5), (0, rows - both.shape[2])))


def kernel(scale, e_ref, t_ref, c_ref, out_ref, pq, acc):
    planes, rows, columns = e_ref.shape

    def taps_of(x):
        pq[lax.rem(x, 3)] = jnp.dot(t_ref[...], e_ref[x], preferred_element_type=jnp.float32)

    acc[...] = jnp.zeros_like(acc)
    pq[2] = jnp.zeros(pq.shape[1:], jnp.float32)
    taps_of(0)

    def step(x, carry):
        now, after, before = lax.rem(x, 3), lax.rem(x + 1, 3), lax.rem(x + 2, 3)

        @pl.when(x < planes - 1)
        def _():
            taps_of(x + 1)

        @pl.when(x == planes - 1)
        def _():
            pq[after] = jnp.zeros(pq.shape[1:], jnp.float32)

        last = x == planes - 1
        two = jnp.where(last, 0.0, 2.0)
        four = jnp.where(last, 0.0, 4.0)
        coef = c_ref[x].T
        v = e_ref[x]
        stiff = pq[before, :rows] + pq[after, :rows] + two * pq[now, :rows]
        yk = coef[:, 0:1] * v.astype(jnp.float32) - coef[:, 1:2] * stiff
        mass = pq[before, rows:] + pq[after, rows:] + four * pq[now, rows:]
        ym = coef[:, 2:3] * mass
        dims = (((0,), (0,)), ((), ()))
        acc[:, :columns] += lax.dot_general(v, yk.astype(jnp.bfloat16), dims, preferred_element_type=jnp.float32)
        acc[:, columns:] += lax.dot_general(v, ym.astype(jnp.bfloat16), dims, preferred_element_type=jnp.float32)
        return carry

    lax.fori_loop(0, planes, step, 0)
    for half in range(2):
        m = acc[:, half * columns:(half + 1) * columns]
        out_ref[:, half * columns:(half + 1) * columns] = (m + m.T) * scale


def per_device(eigvecs, material):
    size_x, size_y, size_z, columns = eigvecs.shape
    axes = ("gx", "gy", "gz")
    devices_all = 1
    for axis in axes:
        devices_all *= lax.axis_size(axis)
    total_cells = size_x * size_y * size_z * devices_all
    ext = material
    for axis, dim in (("gz", 3), ("gy", 2), ("gx", 1)):
        ext = jnp.concatenate([ext, upper(ext, axis, dim)], axis=dim)
    rows = -(-((size_y + 1) * (size_z + 1)) // 16) * 16
    coef = coefficients(ext, rows, (size_x, size_y, size_z))
    z_edge = upper(eigvecs, "gz", 2)[:, :, 0]
    y_face = upper(eigvecs, "gy", 1)[:, 0]
    y_edge = upper(z_edge, "gy", 1)
    tail = rows - (size_y + 1) * (size_z + 1)
    plane = jnp.concatenate(
        [eigvecs.reshape(size_x, size_y * size_z, columns), y_face, z_edge, y_edge,
         jnp.zeros((size_x, tail, columns), eigvecs.dtype)], axis=1)
    extended = jnp.concatenate([plane, upper(plane, "gx", 0)], axis=0)
    matrix = jnp.asarray(plane_matrix(size_y, size_z, rows), jnp.bfloat16)
    part = pl.pallas_call(
        functools.partial(kernel, 0.5 / total_cells),
        out_shape=jax.ShapeDtypeStruct((columns, 2 * columns), jnp.float32),
        in_specs=[pl.BlockSpec(memory_space=pltpu.VMEM)] * 3,
        out_specs=pl.BlockSpec(memory_space=pltpu.VMEM),
        scratch_shapes=[
            pltpu.VMEM((3, 2 * rows, columns), jnp.float32),
            pltpu.VMEM((columns, 2 * columns), jnp.float32),
        ],
        compiler_params=pltpu.CompilerParams(vmem_limit_bytes=60 * 1024 * 1024),
    )(extended, matrix, coef)
    summed = part
    for axis in axes:
        summed = lax.psum_scatter(summed, axis, scatter_dimension=0, tiled=True)
    return (summed[:, :columns], summed[:, columns:])


def solution(mesh):
    return jax.shard_map(
        per_device,
        mesh=mesh,
        in_specs=(P("gx", "gy", "gz", None), P(None, "gx", "gy", "gz")),
        out_specs=(P(("gx", "gy", "gz"), None), P(("gx", "gy", "gz"), None)),
        check_vma=False,
    )
```

```python
import functools
import numpy as np
import jax
import jax.numpy as jnp
from jax import lax
from jax.experimental import pallas as pl
from jax.experimental.pallas import tpu as pltpu
from jax.sharding import PartitionSpec as P


def upper(cells, axis, dim):
    count = lax.axis_size(axis)
    head = lax.slice_in_dim(cells, 0, 1, axis=dim)
    return lax.ppermute(head, axis, [(i + 1, i) for i in range(count - 1)])


def taps(count, middle):
    t = middle * np.eye(count) + np.eye(count, k=1) + np.eye(count, k=-1)
    t[-1, -1] = 0.0
    return t


def rows_of(size_y, size_z):
    order = np.zeros((size_y + 1, size_z + 1), np.int64)
    for y in range(size_y + 1):
        order[y, :size_z] = y * size_z + np.arange(size_z)
        order[y, size_z] = (size_y + 1) * size_z + y
    return order


def plane_matrix(size_y, size_z, rows):
    order = rows_of(size_y, size_z).reshape(-1)
    blocks = []
    for middle in (2.0, 4.0):
        full = np.kron(taps(size_y + 1, middle), taps(size_z + 1, middle))
        block = np.zeros((rows, rows))
        block[np.ix_(order, order)] = full
        blocks.append(block)
    return np.concatenate(blocks, 0)


def coefficients(ext, rows, cells_shape):
    size_x, size_y, size_z = cells_shape
    kappa, rho = ext[0], ext[1]
    field = kappa
    for dim in range(3):
        n = field.shape[dim]
        pad = [(1, 1) if d == dim else (0, 0) for d in range(3)]
        wide = jnp.pad(field, pad)
        lower = lax.slice_in_dim(wide, 0, n, axis=dim)
        above = lax.slice_in_dim(wide, 2, n + 2, axis=dim)
        shape = [1, 1, 1]
        shape[dim] = n
        diag = jnp.asarray(np.r_[np.full(n - 1, 2.0), 0.0].reshape(shape), jnp.float32)
        field = lower + above + diag * field
    owned = np.zeros(kappa.shape, np.float32)
    owned[:size_x, :size_y, :size_z] = 2.0
    diag = owned * kappa + field * (1.0 / 32.0)
    parts = jnp.stack([diag, kappa * (1.0 / 16.0), rho * (1.0 / 216.0)], axis=1)
    main = parts[..., :size_z].reshape(size_x + 1, 3, (size_y + 1) * size_z)
    edge = parts[..., size_z]
    both = jnp.concatenate([main, edge], axis=2)
    return jnp.pad(both, ((0, 0), (0, 5), (0, rows - both.shape[2])))


def kernel(scale, e_ref, t_ref, c_ref, out_ref, pq, acc):
    planes, rows, columns = e_ref.shape

    def taps_of(x):
        pq[lax.rem(x, 3)] = jnp.dot(t_ref[...], e_ref[x], preferred_element_type=jnp.float32)

    acc[...] = jnp.zeros_like(acc)
    pq[2] = jnp.zeros(pq.shape[1:], jnp.float32)
    taps_of(0)

    def step(x, carry):
        now, after, before = lax.rem(x, 3), lax.rem(x + 1, 3), lax.rem(x + 2, 3)

        @pl.when(x < planes - 1)
        def _():
            taps_of(x + 1)

        @pl.when(x == planes - 1)
        def _():
            pq[after] = jnp.zeros(pq.shape[1:], jnp.float32)

        last = x == planes - 1
        two = jnp.where(last, 0.0, 2.0)
        four = jnp.where(last, 0.0, 4.0)
        coef = c_ref[x].T
        v = e_ref[x]
        stiff = pq[before, :rows] + pq[after, :rows] + two * pq[now, :rows]
        yk = coef[:, 0:1] * v.astype(jnp.float32) - coef[:, 1:2] * stiff
        mass = pq[before, rows:] + pq[after, rows:] + four * pq[now, rows:]
        ym = coef[:, 2:3] * mass
        dims = (((0,), (0,)), ((), ()))
        acc[:, :columns] += lax.dot_general(v, yk.astype(jnp.bfloat16), dims, preferred_element_type=jnp.float32)
        acc[:, columns:] += lax.dot_general(v, ym.astype(jnp.bfloat16), dims, preferred_element_type=jnp.float32)
        return carry

    lax.fori_loop(0, planes, step, 0)
    for half in range(2):
        m = acc[:, half * columns:(half + 1) * columns]
        out_ref[:, half * columns:(half + 1) * columns] = (m + m.T) * scale


def spread(axis, piece, landing, send, recv):
    count = lax.axis_size(axis)
    me = lax.axis_index(axis)
    copies = []
    for k in range(1, count):
        peer = lax.rem(me + k, count)
        copy = pltpu.make_async_remote_copy(
            src_ref=piece(peer), dst_ref=landing.at[k - 1],
            send_sem=send.at[k - 1], recv_sem=recv.at[k - 1],
            device_id={axis: peer}, device_id_type=pl.DeviceIdType.MESH)
        copy.start()
        copies.append(copy)
    return copies


def greet(axes):
    barrier = pltpu.get_barrier_semaphore()
    total = 0
    for axis in axes:
        count = lax.axis_size(axis)
        me = lax.axis_index(axis)
        for k in range(1, count):
            pl.semaphore_signal(barrier, inc=1, device_id={axis: lax.rem(me + k, count)},
                                device_id_type=pl.DeviceIdType.MESH)
        total += count - 1
    pl.semaphore_wait(barrier, total)


def reduce_kernel(cut, part, stiff_out, mass_out, rz, sa, sb, ra1, rb1, ta, tb, ra2, rb2, out,
                  *sems):
    z_send, z_recv, a1s, a1r, b1s, b1r, a2s, a2r, b2s, b2r = sems
    gx, gy, gz = (lax.axis_index(a) for a in ("gx", "gy", "gz"))
    greet(("gx", "gy", "gz"))
    first = spread("gz", lambda p: part.at[:, :, p], rz, z_send, z_recv)
    for copy in first:
        copy.wait_recv()
    held = part[:, :, gz]
    for k in range(len(first)):
        held = held + rz[k]
    sa[...] = held[..., :cut]
    sb[...] = held[..., cut:]
    a1 = spread("gy", lambda p: sa.at[:, p], ra1, a1s, a1r)
    b1 = spread("gx", lambda p: sb.at[p], rb1, b1s, b1r)
    for copy in a1:
        copy.wait_recv()
    held = sa[:, gy]
    for k in range(len(a1)):
        held = held + ra1[k]
    ta[...] = held
    a2 = spread("gx", lambda p: ta.at[p], ra2, a2s, a2r)
    for copy in b1:
        copy.wait_recv()
    held = sb[gx]
    for k in range(len(b1)):
        held = held + rb1[k]
    tb[...] = held
    b2 = spread("gy", lambda p: tb.at[p], rb2, b2s, b2r)
    for copy in a2:
        copy.wait_recv()
    held = ta[gx]
    for k in range(len(a2)):
        held = held + ra2[k]
    out[:, :cut] = held
    for copy in b2:
        copy.wait_recv()
    held = tb[gy]
    for k in range(len(b2)):
        held = held + rb2[k]
    out[:, cut:] = held
    columns = stiff_out.shape[1]
    stiff_out[...] = out[:, :columns]
    mass_out[...] = out[:, columns:]
    for copy in first + a1 + b1 + a2 + b2:
        copy.wait_send()


def reduced(part):
    nx, ny, nz = (lax.axis_size(a) for a in ("gx", "gy", "gz"))
    wide = part.shape[1]
    rows = part.shape[0] // (nx * ny * nz)
    cut = (wide * 5 // 8) // 128 * 128
    rest = wide - cut
    f32 = jnp.float32
    dma = pltpu.SemaphoreType.DMA
    vmem = pl.BlockSpec(memory_space=pltpu.VMEM)
    return pl.pallas_call(
        functools.partial(reduce_kernel, cut),
        out_shape=[jax.ShapeDtypeStruct((rows, wide // 2), f32)] * 2,
        in_specs=[vmem],
        out_specs=[vmem, vmem],
        scratch_shapes=[
            pltpu.VMEM((nz - 1, nx, ny, rows, wide), f32),
            pltpu.VMEM((nx, ny, rows, cut), f32),
            pltpu.VMEM((nx, ny, rows, rest), f32),
            pltpu.VMEM((ny - 1, nx, rows, cut), f32),
            pltpu.VMEM((nx - 1, ny, rows, rest), f32),
            pltpu.VMEM((nx, rows, cut), f32),
            pltpu.VMEM((ny, rows, rest), f32),
            pltpu.VMEM((nx - 1, rows, cut), f32),
            pltpu.VMEM((ny - 1, rows, rest), f32),
            pltpu.VMEM((rows, wide), f32),
        ] + [dma((n - 1,)) for n in (nz, nz, ny, ny, nx, nx, nx, nx, ny, ny)],
        compiler_params=pltpu.CompilerParams(collective_id=1, has_side_effects=True),
    )(part.reshape(nx, ny, nz, rows, wide))


def per_device(eigvecs, material):
    size_x, size_y, size_z, columns = eigvecs.shape
    axes = ("gx", "gy", "gz")
    devices_all = 1
    for axis in axes:
        devices_all *= lax.axis_size(axis)
    total_cells = size_x * size_y * size_z * devices_all
    ext = material
    for axis, dim in (("gz", 3), ("gy", 2), ("gx", 1)):
        ext = jnp.concatenate([ext, upper(ext, axis, dim)], axis=dim)
    rows = -(-((size_y + 1) * (size_z + 1)) // 16) * 16
    coef = coefficients(ext, rows, (size_x, size_y, size_z))
    z_edge = upper(eigvecs, "gz", 2)[:, :, 0]
    y_face = upper(eigvecs, "gy", 1)[:, 0]
    y_edge = upper(z_edge, "gy", 1)
    tail = rows - (size_y + 1) * (size_z + 1)
    plane = jnp.concatenate(
        [eigvecs.reshape(size_x, size_y * size_z, columns), y_face, z_edge, y_edge,
         jnp.zeros((size_x, tail, columns), eigvecs.dtype)], axis=1)
    extended = jnp.concatenate([plane, upper(plane, "gx", 0)], axis=0)
    matrix = jnp.asarray(plane_matrix(size_y, size_z, rows), jnp.bfloat16)
    part = pl.pallas_call(
        functools.partial(kernel, 0.5 / total_cells),
        out_shape=jax.ShapeDtypeStruct((columns, 2 * columns), jnp.float32),
        in_specs=[pl.BlockSpec(memory_space=pltpu.VMEM)] * 3,
        out_specs=pl.BlockSpec(memory_space=pltpu.VMEM),
        scratch_shapes=[
            pltpu.VMEM((3, 2 * rows, columns), jnp.float32),
            pltpu.VMEM((columns, 2 * columns), jnp.float32),
        ],
        compiler_params=pltpu.CompilerParams(vmem_limit_bytes=60 * 1024 * 1024),
    )(extended, matrix, coef)
    return tuple(reduced(part))


def solution(mesh):
    return jax.shard_map(
        per_device,
        mesh=mesh,
        in_specs=(P("gx", "gy", "gz", None), P(None, "gx", "gy", "gz")),
        out_specs=(P(("gx", "gy", "gz"), None), P(("gx", "gy", "gz"), None)),
        check_vma=False,
    )
```

```python
import functools
import numpy as np
import jax
import jax.numpy as jnp
from jax import lax
from jax.experimental import pallas as pl
from jax.experimental.pallas import tpu as pltpu
from jax.sharding import PartitionSpec as P


def upper(cells, axis, dim):
    count = lax.axis_size(axis)
    head = lax.slice_in_dim(cells, 0, 1, axis=dim)
    return lax.ppermute(head, axis, [(i + 1, i) for i in range(count - 1)])


def taps(count, middle):
    t = middle * np.eye(count) + np.eye(count, k=1) + np.eye(count, k=-1)
    t[-1, -1] = 0.0
    return t


def rows_of(size_y, size_z):
    order = np.zeros((size_y + 1, size_z + 1), np.int64)
    base = (size_y + 1) * size_z
    for y in range(size_y + 1):
        order[y, :size_z] = y * size_z + np.arange(size_z)
        order[y, size_z] = base + y
    order[size_y, size_z] = base + -(-size_y // 16) * 16
    return order


def plane_matrix(size_y, size_z, rows):
    order = rows_of(size_y, size_z).reshape(-1)
    blocks = []
    for middle in (2.0, 4.0):
        full = np.kron(taps(size_y + 1, middle), taps(size_z + 1, middle))
        block = np.zeros((rows, rows))
        block[np.ix_(order, order)] = full
        blocks.append(block)
    return np.concatenate(blocks, 0)


def coefficients(ext, rows, cells_shape):
    size_x, size_y, size_z = cells_shape
    kappa, rho = ext[0], ext[1]
    field = kappa
    for dim in range(3):
        n = field.shape[dim]
        pad = [(1, 1) if d == dim else (0, 0) for d in range(3)]
        wide = jnp.pad(field, pad)
        lower = lax.slice_in_dim(wide, 0, n, axis=dim)
        above = lax.slice_in_dim(wide, 2, n + 2, axis=dim)
        shape = [1, 1, 1]
        shape[dim] = n
        diag = jnp.asarray(np.r_[np.full(n - 1, 2.0), 0.0].reshape(shape), jnp.float32)
        field = lower + above + diag * field
    owned = np.zeros(kappa.shape, np.float32)
    owned[:size_x, :size_y, :size_z] = 2.0
    diag = owned * kappa + field * (1.0 / 32.0)
    parts = jnp.stack([diag, kappa * (1.0 / 16.0), rho * (1.0 / 216.0)], axis=1)
    main = parts[..., :size_z].reshape(size_x + 1, 3, (size_y + 1) * size_z)
    edge = parts[:, :, :size_y, size_z]
    edge = jnp.pad(edge, ((0, 0), (0, 0), (0, -size_y % 16)))
    both = jnp.concatenate([main, edge, parts[:, :, size_y:, size_z]], axis=2)
    return jnp.pad(both, ((0, 0), (0, 5), (0, rows - both.shape[2])))


OFFSETS = [(0, 1, 0), (0, 0, 1), (1, 0, 0), (0, 1, 1), (1, 0, 1), (1, 1, 0), (1, 1, 1)]
AXES = ("gx", "gy", "gz")


def inside(offset, sign):
    ok = None
    for axis, d in zip(AXES, offset):
        if d:
            at = lax.axis_index(axis)
            here = at > 0 if sign < 0 else at < lax.axis_size(axis) - 1
            ok = here if ok is None else jnp.logical_and(ok, here)
    return ok


def device_at(offset, sign):
    return {axis: lax.axis_index(axis) + sign * d for axis, d in zip(AXES, offset) if d}


def greet_around():
    barrier = pltpu.get_barrier_semaphore()
    total = jnp.int32(0)
    for offset in OFFSETS:
        for sign in (-1, 1):
            there = inside(offset, sign)

            @pl.when(there)
            def _(offset=offset, sign=sign):
                pl.semaphore_signal(barrier, inc=1, device_id=device_at(offset, sign),
                                    device_id_type=pl.DeviceIdType.MESH)

            total = total + jnp.where(there, 1, 0)
    pl.semaphore_wait(barrier, total)


def kernel(scale, v_ref, z_ref, k_ref, t_ref, c_ref, out_ref, e_ref, corners, pq, acc,
           own_sem, send, recv):
    planes, rows, columns = e_ref.shape
    nx, owned, _ = v_ref.shape
    edge = z_ref.shape[1]
    width = rows - owned - edge - 16
    y_at, z_at, c_at = owned, owned + width, owned + width + edge
    own = pltpu.make_async_copy(v_ref, e_ref.at[:nx, :owned], own_sem)
    own.start()
    places = {
        (0, 1, 0): (v_ref.at[:, :width], e_ref.at[:nx, y_at:z_at]),
        (0, 0, 1): (z_ref, e_ref.at[:nx, z_at:c_at]),
        (0, 1, 1): (k_ref, corners.at[0]),
        (1, 0, 0): (v_ref.at[0], e_ref.at[nx, :owned]),
        (1, 0, 1): (z_ref.at[0], e_ref.at[nx, z_at:c_at]),
        (1, 1, 0): (v_ref.at[0, :width], e_ref.at[nx, y_at:z_at]),
        (1, 1, 1): (k_ref, corners.at[1]),
    }
    greet_around()
    copies = {}
    for n, offset in enumerate(OFFSETS):
        src, dst = places[offset]
        copies[offset] = pltpu.make_async_remote_copy(
            src_ref=src, dst_ref=dst, send_sem=send.at[n], recv_sem=recv.at[n],
            device_id=device_at(offset, -1), device_id_type=pl.DeviceIdType.MESH)
        pl.when(inside(offset, -1))(copies[offset].start)
    for offset in OFFSETS:
        src, dst = places[offset]

        @pl.when(jnp.logical_not(inside(offset, 1)))
        def _(dst=dst):
            dst[...] = jnp.zeros(dst.shape, dst.dtype)

    own.wait()
    for offset in OFFSETS:
        pl.when(inside(offset, 1))(copies[offset].wait_recv)
    for x in range(planes):
        row = corners[0, x:x + 1] if x < nx else corners[1, 0:1]
        e_ref[x, c_at:] = jnp.broadcast_to(row.astype(jnp.float32), (16, columns)).astype(e_ref.dtype)

    def taps_of(x):
        pq[lax.rem(x, 3)] = jnp.dot(t_ref[...], e_ref[x], preferred_element_type=jnp.float32)

    acc[...] = jnp.zeros_like(acc)
    pq[2] = jnp.zeros(pq.shape[1:], jnp.float32)
    taps_of(0)

    def step(x, carry):
        now, after, before = lax.rem(x, 3), lax.rem(x + 1, 3), lax.rem(x + 2, 3)

        @pl.when(x < planes - 1)
        def _():
            taps_of(x + 1)

        @pl.when(x == planes - 1)
        def _():
            pq[after] = jnp.zeros(pq.shape[1:], jnp.float32)

        last = x == planes - 1
        two = jnp.where(last, 0.0, 2.0)
        four = jnp.where(last, 0.0, 4.0)
        coef = c_ref[x].T
        v = e_ref[x]
        stiff = pq[before, :rows] + pq[after, :rows] + two * pq[now, :rows]
        yk = coef[:, 0:1] * v.astype(jnp.float32) - coef[:, 1:2] * stiff
        mass = pq[before, rows:] + pq[after, rows:] + four * pq[now, rows:]
        ym = coef[:, 2:3] * mass
        dims = (((0,), (0,)), ((), ()))
        acc[:, :columns] += lax.dot_general(v, yk.astype(jnp.bfloat16), dims, preferred_element_type=jnp.float32)
        acc[:, columns:] += lax.dot_general(v, ym.astype(jnp.bfloat16), dims, preferred_element_type=jnp.float32)
        return carry

    lax.fori_loop(0, planes, step, 0)
    for half in range(2):
        m = acc[:, half * columns:(half + 1) * columns]
        out_ref[:, half * columns:(half + 1) * columns] = (m + m.T) * scale
    for offset in OFFSETS:
        pl.when(inside(offset, -1))(copies[offset].wait_send)


def spread(axis, piece, landing, send, recv):
    count = lax.axis_size(axis)
    me = lax.axis_index(axis)
    copies = []
    for k in range(1, count):
        peer = lax.rem(me + k, count)
        copy = pltpu.make_async_remote_copy(
            src_ref=piece(peer), dst_ref=landing.at[k - 1],
            send_sem=send.at[k - 1], recv_sem=recv.at[k - 1],
            device_id={axis: peer}, device_id_type=pl.DeviceIdType.MESH)
        copy.start()
        copies.append(copy)
    return copies


def greet(axes):
    barrier = pltpu.get_barrier_semaphore()
    total = 0
    for axis in axes:
        count = lax.axis_size(axis)
        me = lax.axis_index(axis)
        for k in range(1, count):
            pl.semaphore_signal(barrier, inc=1, device_id={axis: lax.rem(me + k, count)},
                                device_id_type=pl.DeviceIdType.MESH)
        total += count - 1
    pl.semaphore_wait(barrier, total)


def reduce_kernel(cut, part, stiff_out, mass_out, rz, sa, sb, ra1, rb1, ta, tb, ra2, rb2, out,
                  *sems):
    z_send, z_recv, a1s, a1r, b1s, b1r, a2s, a2r, b2s, b2r = sems
    gx, gy, gz = (lax.axis_index(a) for a in ("gx", "gy", "gz"))
    greet(("gx", "gy", "gz"))
    first = spread("gz", lambda p: part.at[:, :, p], rz, z_send, z_recv)
    for copy in first:
        copy.wait_recv()
    held = part[:, :, gz]
    for k in range(len(first)):
        held = held + rz[k]
    sa[...] = held[..., :cut]
    sb[...] = held[..., cut:]
    a1 = spread("gy", lambda p: sa.at[:, p], ra1, a1s, a1r)
    b1 = spread("gx", lambda p: sb.at[p], rb1, b1s, b1r)
    for copy in a1:
        copy.wait_recv()
    held = sa[:, gy]
    for k in range(len(a1)):
        held = held + ra1[k]
    ta[...] = held
    a2 = spread("gx", lambda p: ta.at[p], ra2, a2s, a2r)
    for copy in b1:
        copy.wait_recv()
    held = sb[gx]
    for k in range(len(b1)):
        held = held + rb1[k]
    tb[...] = held
    b2 = spread("gy", lambda p: tb.at[p], rb2, b2s, b2r)
    for copy in a2:
        copy.wait_recv()
    held = ta[gx]
    for k in range(len(a2)):
        held = held + ra2[k]
    out[:, :cut] = held
    for copy in b2:
        copy.wait_recv()
    held = tb[gy]
    for k in range(len(b2)):
        held = held + rb2[k]
    out[:, cut:] = held
    columns = stiff_out.shape[1]
    stiff_out[...] = out[:, :columns]
    mass_out[...] = out[:, columns:]
    for copy in first + a1 + b1 + a2 + b2:
        copy.wait_send()


def reduced(part):
    nx, ny, nz = (lax.axis_size(a) for a in ("gx", "gy", "gz"))
    wide = part.shape[1]
    rows = part.shape[0] // (nx * ny * nz)
    cut = (wide * 5 // 8) // 128 * 128
    rest = wide - cut
    f32 = jnp.float32
    dma = pltpu.SemaphoreType.DMA
    vmem = pl.BlockSpec(memory_space=pltpu.VMEM)
    return pl.pallas_call(
        functools.partial(reduce_kernel, cut),
        out_shape=[jax.ShapeDtypeStruct((rows, wide // 2), f32)] * 2,
        in_specs=[vmem],
        out_specs=[vmem, vmem],
        scratch_shapes=[
            pltpu.VMEM((nz - 1, nx, ny, rows, wide), f32),
            pltpu.VMEM((nx, ny, rows, cut), f32),
            pltpu.VMEM((nx, ny, rows, rest), f32),
            pltpu.VMEM((ny - 1, nx, rows, cut), f32),
            pltpu.VMEM((nx - 1, ny, rows, rest), f32),
            pltpu.VMEM((nx, rows, cut), f32),
            pltpu.VMEM((ny, rows, rest), f32),
            pltpu.VMEM((nx - 1, rows, cut), f32),
            pltpu.VMEM((ny - 1, rows, rest), f32),
            pltpu.VMEM((rows, wide), f32),
        ] + [dma((n - 1,)) for n in (nz, nz, ny, ny, nx, nx, nx, nx, ny, ny)],
        compiler_params=pltpu.CompilerParams(collective_id=1, has_side_effects=True),
    )(part.reshape(nx, ny, nz, rows, wide))


def per_device(eigvecs, material):
    size_x, size_y, size_z, columns = eigvecs.shape
    axes = ("gx", "gy", "gz")
    devices_all = 1
    for axis in axes:
        devices_all *= lax.axis_size(axis)
    total_cells = size_x * size_y * size_z * devices_all
    ext = material
    for axis, dim in (("gz", 3), ("gy", 2), ("gx", 1)):
        ext = jnp.concatenate([ext, upper(ext, axis, dim)], axis=dim)
    edge = -(-size_y // 16) * 16
    rows = (size_y + 1) * size_z + edge + 16
    coef = coefficients(ext, rows, (size_x, size_y, size_z))
    z_layer = jnp.pad(eigvecs[:, :, 0], ((0, 0), (0, edge - size_y), (0, 0)))
    corner = eigvecs[:, 0, 0]
    matrix = jnp.asarray(plane_matrix(size_y, size_z, rows), jnp.bfloat16)
    vmem = pl.BlockSpec(memory_space=pltpu.VMEM)
    anywhere = pl.BlockSpec(memory_space=pl.ANY)
    part = pl.pallas_call(
        functools.partial(kernel, 0.5 / total_cells),
        out_shape=jax.ShapeDtypeStruct((columns, 2 * columns), jnp.float32),
        in_specs=[anywhere, vmem, vmem, vmem, vmem],
        out_specs=vmem,
        scratch_shapes=[
            pltpu.VMEM((size_x + 1, rows, columns), eigvecs.dtype),
            pltpu.VMEM((2, size_x, columns), eigvecs.dtype),
            pltpu.VMEM((3, 2 * rows, columns), jnp.float32),
            pltpu.VMEM((columns, 2 * columns), jnp.float32),
            pltpu.SemaphoreType.DMA,
            pltpu.SemaphoreType.DMA((7,)),
            pltpu.SemaphoreType.DMA((7,)),
        ],
        compiler_params=pltpu.CompilerParams(
            vmem_limit_bytes=60 * 1024 * 1024, collective_id=0, has_side_effects=True),
    )(eigvecs.reshape(size_x, size_y * size_z, columns), z_layer, corner, matrix, coef)
    return tuple(reduced(part))


def solution(mesh):
    return jax.shard_map(
        per_device,
        mesh=mesh,
        in_specs=(P("gx", "gy", "gz", None), P(None, "gx", "gy", "gz")),
        out_specs=(P(("gx", "gy", "gz"), None), P(("gx", "gy", "gz"), None)),
        check_vma=False,
    )
```

```python
import functools
import numpy as np
import jax
import jax.numpy as jnp
from jax import lax
from jax.experimental import pallas as pl
from jax.experimental.pallas import tpu as pltpu
from jax.sharding import PartitionSpec as P


def upper(cells, axis, dim):
    count = lax.axis_size(axis)
    head = lax.slice_in_dim(cells, 0, 1, axis=dim)
    return lax.ppermute(head, axis, [(i + 1, i) for i in range(count - 1)])


def taps(count, middle):
    t = middle * np.eye(count) + np.eye(count, k=1) + np.eye(count, k=-1)
    t[-1, -1] = 0.0
    return t


def rows_of(size_y, size_z):
    order = np.zeros((size_y + 1, size_z + 1), np.int64)
    base = (size_y + 1) * size_z
    for y in range(size_y + 1):
        order[y, :size_z] = y * size_z + np.arange(size_z)
        order[y, size_z] = base + y
    order[size_y, size_z] = base + -(-size_y // 16) * 16
    return order


def plane_matrix(size_y, size_z, rows):
    order = rows_of(size_y, size_z).reshape(-1)
    blocks = []
    for middle in (2.0, 4.0):
        full = np.kron(taps(size_y + 1, middle), taps(size_z + 1, middle))
        block = np.zeros((rows, rows))
        block[np.ix_(order, order)] = full
        blocks.append(block)
    return np.concatenate(blocks, 0)


def coefficients(ext, rows, cells_shape):
    size_x, size_y, size_z = cells_shape
    kappa, rho = ext[0], ext[1]
    field = kappa
    for dim in range(3):
        n = field.shape[dim]
        pad = [(1, 1) if d == dim else (0, 0) for d in range(3)]
        wide = jnp.pad(field, pad)
        lower = lax.slice_in_dim(wide, 0, n, axis=dim)
        above = lax.slice_in_dim(wide, 2, n + 2, axis=dim)
        shape = [1, 1, 1]
        shape[dim] = n
        diag = jnp.asarray(np.r_[np.full(n - 1, 2.0), 0.0].reshape(shape), jnp.float32)
        field = lower + above + diag * field
    owned = np.zeros(kappa.shape, np.float32)
    owned[:size_x, :size_y, :size_z] = 2.0
    diag = owned * kappa + field * (1.0 / 32.0)
    parts = jnp.stack([diag, kappa * (1.0 / 16.0), rho * (1.0 / 216.0)], axis=1)
    main = parts[..., :size_z].reshape(size_x + 1, 3, (size_y + 1) * size_z)
    edge = parts[:, :, :size_y, size_z]
    edge = jnp.pad(edge, ((0, 0), (0, 0), (0, -size_y % 16)))
    both = jnp.concatenate([main, edge, parts[:, :, size_y:, size_z]], axis=2)
    return jnp.pad(both, ((0, 0), (0, 5), (0, rows - both.shape[2])))


OFFSETS = [(0, 1, 0), (0, 0, 1), (1, 0, 0), (0, 1, 1), (1, 0, 1), (1, 1, 0), (1, 1, 1)]
AXES = ("gx", "gy", "gz")


def inside(offset, sign):
    ok = None
    for axis, d in zip(AXES, offset):
        if d:
            at = lax.axis_index(axis)
            here = at > 0 if sign < 0 else at < lax.axis_size(axis) - 1
            ok = here if ok is None else jnp.logical_and(ok, here)
    return ok


def device_at(offset, sign):
    return {axis: lax.axis_index(axis) + sign * d for axis, d in zip(AXES, offset) if d}


def greet_around():
    barrier = pltpu.get_barrier_semaphore()
    total = jnp.int32(0)
    for offset in OFFSETS:
        for sign in (-1, 1):
            there = inside(offset, sign)

            @pl.when(there)
            def _(offset=offset, sign=sign):
                pl.semaphore_signal(barrier, inc=1, device_id=device_at(offset, sign),
                                    device_id_type=pl.DeviceIdType.MESH)

            total = total + jnp.where(there, 1, 0)
    pl.semaphore_wait(barrier, total)


def kernel(scale, v_ref, z_ref, k_ref, t_ref, c_ref, out_ref, e_ref, corners, p0, p1, p2, p3, acc,
           own_sem, send, recv):
    slots = (p0, p1, p2, p3)
    rows, columns = e_ref.shape[1:]
    nx, owned, _ = v_ref.shape
    planes = nx + 1
    edge = z_ref.shape[1]
    width = rows - owned - edge - 16
    y_at, z_at, c_at = owned, owned + width, owned + width + edge
    own = pltpu.make_async_copy(v_ref, e_ref.at[:nx, :owned], own_sem)
    own.start()
    places = {
        (0, 1, 0): (v_ref.at[:, :width], e_ref.at[:nx, y_at:z_at]),
        (0, 0, 1): (z_ref, e_ref.at[:nx, z_at:c_at]),
        (0, 1, 1): (k_ref, corners.at[0]),
        (1, 0, 0): (v_ref.at[0], e_ref.at[nx, :owned]),
        (1, 0, 1): (z_ref.at[0], e_ref.at[nx, z_at:c_at]),
        (1, 1, 0): (v_ref.at[0, :width], e_ref.at[nx, y_at:z_at]),
        (1, 1, 1): (k_ref, corners.at[1]),
    }
    greet_around()
    copies = {}
    for n, offset in enumerate(OFFSETS):
        src, dst = places[offset]
        copies[offset] = pltpu.make_async_remote_copy(
            src_ref=src, dst_ref=dst, send_sem=send.at[n], recv_sem=recv.at[n],
            device_id=device_at(offset, -1), device_id_type=pl.DeviceIdType.MESH)
        pl.when(inside(offset, -1))(copies[offset].start)
    for offset in OFFSETS:
        src, dst = places[offset]

        @pl.when(jnp.logical_not(inside(offset, 1)))
        def _(dst=dst):
            dst[...] = jnp.zeros(dst.shape, dst.dtype)

    own.wait()
    for offset in OFFSETS:
        pl.when(inside(offset, 1))(copies[offset].wait_recv)
    for x in range(planes):
        row = corners[0, x:x + 1] if x < nx else corners[1, 0:1]
        e_ref[x, c_at:] = jnp.broadcast_to(row.astype(jnp.float32), (16, columns)).astype(e_ref.dtype)

    def taps_of(x, slot):
        slots[slot % 4][...] = jnp.dot(t_ref[...], e_ref[x], preferred_element_type=jnp.float32)

    def step(x, slot, two, four, ahead):
        if ahead:
            taps_of(x + 2, slot + 2)
        before, now, after = (slots[(slot + k) % 4] for k in (3, 0, 1))
        coef = c_ref[x].T
        v = e_ref[x]
        stiff = before[:rows] + after[:rows] + two * now[:rows]
        yk = coef[:, 0:1] * v.astype(jnp.float32) - coef[:, 1:2] * stiff
        mass = before[rows:] + after[rows:] + four * now[rows:]
        ym = coef[:, 2:3] * mass
        dims = (((0,), (0,)), ((), ()))
        acc[:, :columns] += lax.dot_general(v, yk.astype(jnp.bfloat16), dims, preferred_element_type=jnp.float32)
        acc[:, columns:] += lax.dot_general(v, ym.astype(jnp.bfloat16), dims, preferred_element_type=jnp.float32)

    acc[...] = jnp.zeros_like(acc)
    e_ref[planes] = jnp.zeros((rows, columns), e_ref.dtype)
    p3[...] = jnp.zeros_like(p3)
    taps_of(0, 0)
    taps_of(1, 1)
    whole = (planes - 1) // 4

    def four_steps(i, carry):
        for j in range(4):
            step(4 * i + j, j, 2.0, 4.0, True)
        return carry

    lax.fori_loop(0, whole, four_steps, 0)
    for x in range(4 * whole, planes):
        last = x == planes - 1
        step(x, x, 0.0 if last else 2.0, 0.0 if last else 4.0, x + 2 <= planes)
    for half in range(2):
        m = acc[:, half * columns:(half + 1) * columns]
        out_ref[:, half * columns:(half + 1) * columns] = (m + m.T) * scale
    for offset in OFFSETS:
        pl.when(inside(offset, -1))(copies[offset].wait_send)


def spread(axis, piece, landing, send, recv):
    count = lax.axis_size(axis)
    me = lax.axis_index(axis)
    copies = []
    for k in range(1, count):
        peer = lax.rem(me + k, count)
        copy = pltpu.make_async_remote_copy(
            src_ref=piece(peer), dst_ref=landing.at[k - 1],
            send_sem=send.at[k - 1], recv_sem=recv.at[k - 1],
            device_id={axis: peer}, device_id_type=pl.DeviceIdType.MESH)
        copy.start()
        copies.append(copy)
    return copies


def greet(axes):
    barrier = pltpu.get_barrier_semaphore()
    total = 0
    for axis in axes:
        count = lax.axis_size(axis)
        me = lax.axis_index(axis)
        for k in range(1, count):
            pl.semaphore_signal(barrier, inc=1, device_id={axis: lax.rem(me + k, count)},
                                device_id_type=pl.DeviceIdType.MESH)
        total += count - 1
    pl.semaphore_wait(barrier, total)


def reduce_kernel(cut, part, stiff_out, mass_out, rz, sa, sb, ra1, rb1, ta, tb, ra2, rb2, out,
                  *sems):
    z_send, z_recv, a1s, a1r, b1s, b1r, a2s, a2r, b2s, b2r = sems
    gx, gy, gz = (lax.axis_index(a) for a in ("gx", "gy", "gz"))
    greet(("gx", "gy", "gz"))
    first = spread("gz", lambda p: part.at[:, :, p], rz, z_send, z_recv)
    for copy in first:
        copy.wait_recv()
    held = part[:, :, gz]
    for k in range(len(first)):
        held = held + rz[k]
    sa[...] = held[..., :cut]
    sb[...] = held[..., cut:]
    a1 = spread("gy", lambda p: sa.at[:, p], ra1, a1s, a1r)
    b1 = spread("gx", lambda p: sb.at[p], rb1, b1s, b1r)
    for copy in a1:
        copy.wait_recv()
    held = sa[:, gy]
    for k in range(len(a1)):
        held = held + ra1[k]
    ta[...] = held
    a2 = spread("gx", lambda p: ta.at[p], ra2, a2s, a2r)
    for copy in b1:
        copy.wait_recv()
    held = sb[gx]
    for k in range(len(b1)):
        held = held + rb1[k]
    tb[...] = held
    b2 = spread("gy", lambda p: tb.at[p], rb2, b2s, b2r)
    for copy in a2:
        copy.wait_recv()
    held = ta[gx]
    for k in range(len(a2)):
        held = held + ra2[k]
    out[:, :cut] = held
    for copy in b2:
        copy.wait_recv()
    held = tb[gy]
    for k in range(len(b2)):
        held = held + rb2[k]
    out[:, cut:] = held
    columns = stiff_out.shape[1]
    stiff_out[...] = out[:, :columns]
    mass_out[...] = out[:, columns:]
    for copy in first + a1 + b1 + a2 + b2:
        copy.wait_send()


def reduced(part):
    nx, ny, nz = (lax.axis_size(a) for a in ("gx", "gy", "gz"))
    wide = part.shape[1]
    rows = part.shape[0] // (nx * ny * nz)
    cut = (wide * 5 // 8) // 128 * 128
    rest = wide - cut
    f32 = jnp.float32
    dma = pltpu.SemaphoreType.DMA
    vmem = pl.BlockSpec(memory_space=pltpu.VMEM)
    return pl.pallas_call(
        functools.partial(reduce_kernel, cut),
        out_shape=[jax.ShapeDtypeStruct((rows, wide // 2), f32)] * 2,
        in_specs=[vmem],
        out_specs=[vmem, vmem],
        scratch_shapes=[
            pltpu.VMEM((nz - 1, nx, ny, rows, wide), f32),
            pltpu.VMEM((nx, ny, rows, cut), f32),
            pltpu.VMEM((nx, ny, rows, rest), f32),
            pltpu.VMEM((ny - 1, nx, rows, cut), f32),
            pltpu.VMEM((nx - 1, ny, rows, rest), f32),
            pltpu.VMEM((nx, rows, cut), f32),
            pltpu.VMEM((ny, rows, rest), f32),
            pltpu.VMEM((nx - 1, rows, cut), f32),
            pltpu.VMEM((ny - 1, rows, rest), f32),
            pltpu.VMEM((rows, wide), f32),
        ] + [dma((n - 1,)) for n in (nz, nz, ny, ny, nx, nx, nx, nx, ny, ny)],
        compiler_params=pltpu.CompilerParams(collective_id=1, has_side_effects=True),
    )(part.reshape(nx, ny, nz, rows, wide))


def per_device(eigvecs, material):
    size_x, size_y, size_z, columns = eigvecs.shape
    axes = ("gx", "gy", "gz")
    devices_all = 1
    for axis in axes:
        devices_all *= lax.axis_size(axis)
    total_cells = size_x * size_y * size_z * devices_all
    ext = material
    for axis, dim in (("gz", 3), ("gy", 2), ("gx", 1)):
        ext = jnp.concatenate([ext, upper(ext, axis, dim)], axis=dim)
    edge = -(-size_y // 16) * 16
    rows = (size_y + 1) * size_z + edge + 16
    coef = coefficients(ext, rows, (size_x, size_y, size_z))
    z_layer = jnp.pad(eigvecs[:, :, 0], ((0, 0), (0, edge - size_y), (0, 0)))
    corner = eigvecs[:, 0, 0]
    matrix = jnp.asarray(plane_matrix(size_y, size_z, rows), jnp.bfloat16)
    vmem = pl.BlockSpec(memory_space=pltpu.VMEM)
    anywhere = pl.BlockSpec(memory_space=pl.ANY)
    part = pl.pallas_call(
        functools.partial(kernel, 0.5 / total_cells),
        out_shape=jax.ShapeDtypeStruct((columns, 2 * columns), jnp.float32),
        in_specs=[anywhere, vmem, vmem, vmem, vmem],
        out_specs=vmem,
        scratch_shapes=[
            pltpu.VMEM((size_x + 2, rows, columns), eigvecs.dtype),
            pltpu.VMEM((2, size_x, columns), eigvecs.dtype),
        ] + [pltpu.VMEM((2 * rows, columns), jnp.float32)] * 4 + [
            pltpu.VMEM((columns, 2 * columns), jnp.float32),
            pltpu.SemaphoreType.DMA,
            pltpu.SemaphoreType.DMA((7,)),
            pltpu.SemaphoreType.DMA((7,)),
        ],
        compiler_params=pltpu.CompilerParams(
            vmem_limit_bytes=60 * 1024 * 1024, collective_id=0, has_side_effects=True),
    )(eigvecs.reshape(size_x, size_y * size_z, columns), z_layer, corner, matrix, coef)
    return tuple(reduced(part))


def solution(mesh):
    return jax.shard_map(
        per_device,
        mesh=mesh,
        in_specs=(P("gx", "gy", "gz", None), P(None, "gx", "gy", "gz")),
        out_specs=(P(("gx", "gy", "gz"), None), P(("gx", "gy", "gz"), None)),
        check_vma=False,
    )
```
